32 devices in a mesh: dp: 4 (over y, x), expert: 8 (over z, core).
Axes of the slice: x: 2, y: 2, z: 4, core: 2. Of those that a mesh axis runs over, the one named last changes fastest.
Arguments:
- hidden: bfloat16 [8, 4608, 1408], P('expert', 'dp')
- upstream: bfloat16 [8, 4608, 2048], P('expert', 'dp')
- token_counts: int32 [8, 4], P('expert', 'dp'), may hold values from 1 to 1152, as said below
- master: float32 [8, 1408, 2048], P('expert', 'dp'), may hold values from -0.15625 to 0.15625
- first_moment: float32 [8, 1408, 2048], P('expert', 'dp'), may hold values from -6 to 6
- second_moment: float32 [8, 1408, 2048], P('expert', 'dp'), may hold values from 0.25 to 4
- router_input: bfloat16 [4096, 2048], P(('dp', 'expert')), may hold values from -6 to 6
- router_cot: bfloat16 [64, 4096], P(None, ('dp', 'expert'))
- router_master: float32 [64, 2048], replicated, may hold values from -0.125 to 0.125
- router_first: float32 [64, 2048], replicated, may hold values from -6 to 6
- router_second: float32 [64, 2048], replicated, may hold values from 0.25 to 4
- partner: int32 [8], replicated, may hold values from 0 to 7, as said below
Outputs:
- new_weight: bfloat16 [8, 1408, 2048], P('expert')
- new_master: float32 [8, 1408, 2048], P('expert', 'dp')
- new_first: float32 [8, 1408, 2048], P('expert', 'dp')
- new_second: float32 [8, 1408, 2048], P('expert', 'dp')
- router_master_new: float32 [64, 2048], replicated
- router_first_new: float32 [64, 2048], replicated
- router_second_new: float32 [64, 2048], replicated
The draws below stay inside these ranges and needn't reach their ends.
Inputs may be any that keep to these rules, and one draw needn't show every extreme that they name: partner[partner[p]] = p for every position p; a position with partner[p] = p keeps its expert. The first token_counts[e, d] of replica d's 1152 slots for position e are live, the rest are padding.
All inputs are finite; a program needn't handle non-finite values.
Results may differ from the reference program's by a relative error of at most 0.001.
Values may be sent and summed in bfloat16 or wider, within the bound.
A program may use at most 128 MiB of HBM per device.

```python
import math
import jax
import jax.numpy as jnp
from jax import lax

D = 2048
F = 1408
EXP_ALL = 64
ROWS = 1152
EXPERTS = 8
TOKENS = 4096
N_DP = 4


def draw_hidden(key, part):
    key_base = jax.random.fold_in(key, 11)
    key_column = jax.random.fold_in(key, 12)
    key_row = jax.random.fold_in(key, 13)
    shape_all = (EXPERTS, N_DP * ROWS, F)
    base_values = jax.random.normal(key_base, shape_all, jnp.float32)
    column_rise = jnp.power(3.0, jnp.arange(F, dtype=jnp.float32) / max(F - 1, 1))
    column_scale = jnp.exp(jax.random.uniform(key_column, (F,), jnp.float32, 0.0, math.log(10.0))) * column_rise
    row_scale = jnp.exp(jax.random.uniform(key_row, (EXPERTS, N_DP * ROWS, 1), jnp.float32, 0.0, math.log(4.0)))
    return (0.25 * base_values * row_scale * column_scale).astype(jnp.bfloat16)


def draw_upstream(key, part):
    key_base = jax.random.fold_in(key, 21)
    key_row = jax.random.fold_in(key, 22)
    shape_all = (EXPERTS, N_DP * ROWS, D)
    base_values = jax.random.normal(key_base, shape_all, jnp.float32)
    row_scale = jnp.exp(jax.random.uniform(key_row, (EXPERTS, N_DP * ROWS, 1), jnp.float32, 0.0, math.log(10.0)))
    expert_scale = jnp.power(3.0, jnp.arange(EXPERTS, dtype=jnp.float32) / max(EXPERTS - 1, 1))
    return (0.3 * base_values * row_scale * expert_scale[:, None, None]).astype(jnp.bfloat16)


def draw_router_cot(key, part):
    key_base = jax.random.fold_in(key, 31)
    key_column = jax.random.fold_in(key, 32)
    shape_all = (EXP_ALL, TOKENS)
    base_values = jax.random.normal(key_base, shape_all, jnp.float32)
    token_rise = jnp.power(3.0, jnp.arange(TOKENS, dtype=jnp.float32) / max(TOKENS - 1, 1))
    token_scale = jnp.exp(jax.random.uniform(key_column, (TOKENS,), jnp.float32, 0.0, math.log(10.0))) * token_rise
    return (0.3 * base_values * token_scale).astype(jnp.bfloat16)


def draw_token_counts(key, part):
    key_hot = jax.random.fold_in(key, 41)
    key_light = jax.random.fold_in(key, 42)
    hot_rank = jax.random.permutation(key_hot, EXPERTS)
    is_hot = hot_rank < max(EXPERTS // 4, 1)
    light = jax.random.randint(key_light, (EXPERTS, N_DP), 1, ROWS // 2 + 1)
    return jnp.where(is_hot[:, None], ROWS, light).astype(jnp.int32)


def draw_partner(key, part):
    key_order = jax.random.fold_in(key, 51)
    key_pairs = jax.random.fold_in(key, 52)
    order = jax.random.permutation(key_order, EXPERTS).astype(jnp.int32)
    pair_count = jax.random.randint(key_pairs, (), EXPERTS // 4, EXPERTS // 2 + 1)
    places = jnp.arange(EXPERTS, dtype=jnp.int32)
    mate_place = jnp.where(places < 2 * pair_count, jnp.bitwise_xor(places, 1), places)
    return jnp.zeros((EXPERTS,), jnp.int32).at[order].set(jnp.take(order, mate_place)).astype(jnp.int32)


def block_scale(own_key, shape, shards, low, top_value):
    gain = 1.0
    for axis_at, shards_of in shards:
        draws = jax.random.uniform(jax.random.fold_in(jax.random.fold_in(own_key, 6), axis_at), (shards_of,), jnp.float32, low / len(shards), top_value / len(shards))
        gain = gain * jnp.repeat(jnp.exp(draws), shape[axis_at] // shards_of).reshape((-1,) + (1,) * (len(shape) - 1 - axis_at))
    return gain


def scatter_about(rng, shape, scale, limit, split=(), kind=jnp.bfloat16):
    result = jax.random.normal(rng, shape, jnp.float32) * scale
    if len(split) > 0:
        result = block_scale(rng, shape, split, -0.22, 0.18) * result
    return jnp.clip(result, min=-limit, max=limit).astype(kind)


def setup_inputs(seed: int = 0) -> dict:
    splits = jax.random.split(jax.random.key(seed), 13)
    return {
        "hidden": draw_hidden(jax.random.fold_in(splits[12], 71), 0),
        "upstream": draw_upstream(jax.random.fold_in(splits[12], 71), 0),
        "token_counts": draw_token_counts(jax.random.fold_in(splits[12], 71), 0),
        "master": scatter_about(splits[3], (EXPERTS, F, D), F ** -0.5, 0.15625, ((0, 8), (1, 4)), jnp.float32),
        "first_moment": scatter_about(splits[4], (EXPERTS, F, D), 1.0, 6.0, ((0, 8), (1, 4)), jnp.float32),
        "second_moment": jnp.clip(jnp.exp(math.log(4.0) - 2.7725887 * jax.random.uniform(splits[5], (EXPERTS, F, D), jnp.float32) ** block_scale(splits[5], (EXPERTS, F, D), ((0, 8), (1, 4)), -0.2, 0.2)), 0.25, 4.0),
        "router_input": scatter_about(splits[6], (TOKENS, D), 1.0, 6.0, ((0, 32),)),
        "router_cot": draw_router_cot(jax.random.fold_in(splits[12], 71), 0),
        "router_master": scatter_about(splits[8], (EXP_ALL, D), D ** -0.5, 0.125, (), jnp.float32),
        "router_first": scatter_about(splits[9], (EXP_ALL, D), 1.0, 6.0, (), jnp.float32),
        "router_second": jnp.clip(jnp.exp(jax.random.uniform(splits[10], (EXP_ALL, D), jnp.float32, math.log(0.25), math.log(4.0))), 0.25, 4.0),
        "partner": draw_partner(jax.random.fold_in(splits[12], 71), 0),
    }


beta_first = 0.9
beta_second = 0.95
learn_rate = 0.001
decay_weight = 0.1
adam_eps = 1e-08
norm_eps = 1e-06
correct_first = 1.0 - 0.9 ** 10
correct_second = 1.0 - 0.95 ** 10

def adam_update(gradient, moment_one, moment_two, weights):
    first_new = beta_first * moment_one + (1.0 - beta_first) * gradient
    second_new = beta_second * moment_two + (1.0 - beta_second) * gradient * gradient
    ratio = first_new / correct_first / (jnp.sqrt(second_new / correct_second) + adam_eps)
    weights_new = weights - learn_rate * (ratio + decay_weight * weights)
    return (weights_new, first_new, second_new)

def reference(hidden, upstream, token_counts, master, first_moment, second_moment, router_input, router_cot, router_master, router_first, router_second, partner):
    row_index = jnp.arange(N_DP * ROWS, dtype=jnp.int32)
    within = row_index % ROWS
    replica = row_index // ROWS

    def expert_grad(packed):
        activations, grads_out, counts = packed
        live_rows = within < jnp.take(counts, replica)
        masked = jnp.where(live_rows[:, None], activations, jnp.zeros_like(activations))
        return jnp.dot(masked.T, grads_out, preferred_element_type=jnp.float32)
    gradient = lax.map(expert_grad, (hidden, upstream, token_counts))
    router_grad = jnp.dot(router_cot, router_input, preferred_element_type=jnp.float32)
    total_square = jnp.sum(gradient * gradient) + jnp.sum(router_grad * router_grad)
    clip_limit = 2.0 * math.sqrt(float(EXPERTS * F * D + EXP_ALL * D))
    factor = jnp.minimum(1.0, clip_limit / (jnp.sqrt(total_square) + norm_eps))
    master_new, first_new, second_new = adam_update(factor * gradient, first_moment, second_moment, master)
    router_outs = adam_update(factor * router_grad, router_first, router_second, router_master)
    moved_master = jnp.take(master_new, partner, axis=0)
    moved_first = jnp.take(first_new, partner, axis=0)
    moved_second = jnp.take(second_new, partner, axis=0)
    return (moved_master.astype(jnp.bfloat16), moved_master, moved_first, moved_second, router_outs[0], router_outs[1], router_outs[2])
```

```python
import math

import jax
import jax.numpy as jnp
from jax import lax
from jax.sharding import PartitionSpec as P

beta_first = 0.9
beta_second = 0.95
learn_rate = 0.001
decay_weight = 0.1
adam_eps = 1e-08
norm_eps = 1e-06
correct_first = 1.0 - 0.9**10
correct_second = 1.0 - 0.95**10


def adam_update(gradient, moment_one, moment_two, weights):
    first_new = beta_first * moment_one + (1.0 - beta_first) * gradient
    second_new = beta_second * moment_two + (1.0 - beta_second) * gradient * gradient
    ratio = first_new / correct_first / (jnp.sqrt(second_new / correct_second) + adam_eps)
    weights_new = weights - learn_rate * (ratio + decay_weight * weights)
    return (weights_new, first_new, second_new)


code_top = 32767.0
steps_per_octave = 256.0


def scale_of(level):
    return jnp.exp2(level.astype(jnp.float32) * (1.0 / steps_per_octave))


def encode(blocks):
    groups, rows, width = blocks.shape
    peak = jnp.maximum(jnp.max(jnp.abs(blocks), axis=2), 1e-37)
    level = jnp.clip(jnp.ceil(jnp.log2(peak) * steps_per_octave), -32000.0, 32767.0).astype(jnp.int16)
    scaled = blocks * (code_top / scale_of(level))[:, :, None]
    codes = jnp.clip(jnp.round(scaled), -code_top, code_top).astype(jnp.int16)
    extra = -(-rows // width)
    levels = jnp.pad(level, ((0, 0), (0, extra * width - rows))).reshape(groups, extra, width)
    return jnp.concatenate([codes, levels], axis=1)


def decode(payload, rows):
    groups, _, width = payload.shape
    level = payload[:, rows:].reshape(groups, -1)[:, :rows]
    return payload[:, :rows].astype(jnp.float32) * (scale_of(level) * (1.0 / code_top))[:, :, None]


def to_pieces(matrix, groups):
    rows, width = matrix.shape
    return matrix.reshape(rows, groups, width // groups).swapaxes(0, 1)


def from_pieces(pieces):
    groups, rows, width = pieces.shape
    return pieces.swapaxes(0, 1).reshape(rows, groups * width)


def exchange(payload, axis="expert"):
    return lax.all_to_all(payload, axis, split_axis=0, concat_axis=0, tiled=True)


def regather(weight_shard):
    return lax.all_gather(weight_shard, "dp", axis=0, tiled=True)


def on_device(
    hidden,
    upstream,
    token_counts,
    master,
    first_moment,
    second_moment,
    router_input,
    router_cot,
    router_master,
    router_first,
    router_second,
    partner,
):
    hidden_units = hidden.shape[2]
    features = upstream.shape[2]
    row_count = hidden.shape[1]
    groups = lax.axis_size("expert")
    rows = master.shape[1]
    early_master = exchange(encode(to_pieces(master[0], groups)))
    early_first = exchange(encode(to_pieces(first_moment[0], groups)))
    early_second = exchange(encode(to_pieces(second_moment[0], groups)))
    live_rows = jnp.arange(row_count, dtype=jnp.int32) < token_counts[0, 0]
    activations = hidden[0]
    grads_out = upstream[0]
    masked_out = jnp.where(live_rows[:, None], grads_out, jnp.zeros_like(grads_out))
    router_partial = jnp.dot(router_cot, router_input, preferred_element_type=jnp.float32)
    partial = lax.dot_general(
        activations, masked_out, (((0,), (0,)), ((), ())), preferred_element_type=jnp.float32
    )
    gradient = lax.psum_scatter(partial, "dp", scatter_dimension=0, tiled=True)
    moved_gradient = exchange(encode(to_pieces(gradient, groups)))
    router_grad = lax.psum(router_partial, ("dp", "expert"))
    expert_square = lax.psum(jnp.sum(gradient * gradient), ("dp", "expert"))
    total_square = expert_square + jnp.sum(router_grad * router_grad)
    clip_limit = 2.0 * math.sqrt(
        float(groups * hidden_units * features + router_cot.shape[0] * features)
    )
    factor = jnp.minimum(1.0, clip_limit / (jnp.sqrt(total_square) + norm_eps))
    states = adam_update(
        factor * decode(moved_gradient, rows),
        decode(early_first, rows),
        decode(early_second, rows),
        decode(early_master, rows),
    )
    router_outs = adam_update(factor * router_grad, router_first, router_second, router_master)
    sent = [encode(jnp.take(member, partner, axis=0)) for member in (states[0], states[1], states[2])]
    moved = [from_pieces(decode(exchange(payload), rows)) for payload in sent]
    moved_weight = regather(moved[0].astype(jnp.bfloat16))
    return (
        moved_weight[None],
        moved[0][None],
        moved[1][None],
        moved[2][None],
        router_outs[0],
        router_outs[1],
        router_outs[2],
    )


def solution(mesh):
    in_specs = (
        P("expert", "dp", None),
        P("expert", "dp", None),
        P("expert", "dp"),
        P("expert", "dp", None),
        P("expert", "dp", None),
        P("expert", "dp", None),
        P(("dp", "expert"), None),
        P(None, ("dp", "expert")),
        P(),
        P(),
        P(),
        P(),
    )
    out_specs = (
        P("expert", None, None),
        P("expert", "dp", None),
        P("expert", "dp", None),
        P("expert", "dp", None),
        P(),
        P(),
        P(),
    )
    return jax.shard_map(
        on_device, mesh=mesh, in_specs=in_specs, out_specs=out_specs, check_vma=False
    )
```

```python
import math

import jax
import jax.numpy as jnp
from jax import lax
from jax.sharding import PartitionSpec as P

beta_first = 0.9
beta_second = 0.95
learn_rate = 0.001
decay_weight = 0.1
adam_eps = 1e-08
norm_eps = 1e-06
correct_first = 1.0 - 0.9**10
correct_second = 1.0 - 0.95**10


def adam_update(gradient, moment_one, moment_two, weights):
    first_new = beta_first * moment_one + (1.0 - beta_first) * gradient
    second_new = beta_second * moment_two + (1.0 - beta_second) * gradient * gradient
    ratio = first_new / correct_first / (jnp.sqrt(second_new / correct_second) + adam_eps)
    weights_new = weights - learn_rate * (ratio + decay_weight * weights)
    return (weights_new, first_new, second_new)


code_top = 32767.0
steps_per_octave = 256.0


def scale_of(level):
    return jnp.exp2(level.astype(jnp.float32) * (1.0 / steps_per_octave))


def encode(blocks):
    groups, rows, width = blocks.shape
    peak = jnp.maximum(jnp.max(jnp.abs(blocks), axis=2), 1e-37)
    level = jnp.clip(jnp.ceil(jnp.log2(peak) * steps_per_octave), -32000.0, 32767.0).astype(jnp.int16)
    scaled = blocks * (code_top / scale_of(level))[:, :, None]
    codes = jnp.clip(jnp.round(scaled), -code_top, code_top).astype(jnp.int16)
    extra = -(-rows // width)
    levels = jnp.pad(level, ((0, 0), (0, extra * width - rows))).reshape(groups, extra, width)
    return jnp.concatenate([codes, levels], axis=1)


def decode(payload, rows):
    groups, _, width = payload.shape
    level = payload[:, rows:].reshape(groups, -1)[:, :rows]
    return payload[:, :rows].astype(jnp.float32) * (scale_of(level) * (1.0 / code_top))[:, :, None]


def to_pieces(matrix, groups):
    rows, width = matrix.shape
    return matrix.reshape(rows, groups, width // groups).swapaxes(0, 1)


def from_pieces(pieces):
    groups, rows, width = pieces.shape
    return pieces.swapaxes(0, 1).reshape(rows, groups * width)


def exchange(payload, axis="expert"):
    return lax.all_to_all(payload, axis, split_axis=0, concat_axis=0, tiled=True)


def regather(weight_shard):
    return lax.all_gather(weight_shard, "dp", axis=0, tiled=True)


def on_device(
    hidden,
    upstream,
    token_counts,
    master,
    first_moment,
    second_moment,
    router_input,
    router_cot,
    router_master,
    router_first,
    router_second,
    partner,
):
    hidden_units = hidden.shape[2]
    features = upstream.shape[2]
    row_count = hidden.shape[1]
    groups = lax.axis_size("expert")
    rows = master.shape[1]
    early_master = exchange(encode(to_pieces(master[0], groups)))
    early_first = exchange(encode(to_pieces(first_moment[0], groups)))
    early_second = exchange(encode(to_pieces(second_moment[0], groups)))
    live_rows = jnp.arange(row_count, dtype=jnp.int32) < token_counts[0, 0]
    activations = hidden[0]
    grads_out = upstream[0]
    masked_out = jnp.where(live_rows[:, None], grads_out, jnp.zeros_like(grads_out))
    router_partial = jnp.dot(router_cot, router_input, preferred_element_type=jnp.float32)
    everyone = lax.axis_size("dp") * groups
    router_terms = exchange(router_partial.reshape(everyone, -1), ("dp", "expert"))
    router_share = jnp.sum(router_terms, axis=0)
    partial = lax.dot_general(
        activations, masked_out, (((0,), (0,)), ((), ())), preferred_element_type=jnp.float32
    )
    gradient = lax.psum_scatter(partial, "dp", scatter_dimension=0, tiled=True)
    moved_gradient = exchange(encode(to_pieces(gradient, groups)))
    packet = jnp.concatenate(
        [router_share, jnp.full((128,), jnp.sum(gradient * gradient), jnp.float32)]
    )
    packets = lax.all_gather(packet, ("dp", "expert"), axis=0)
    router_grad = packets[:, : router_share.shape[0]].reshape(router_partial.shape)
    total_square = jnp.sum(packets[:, -1]) + jnp.sum(router_grad * router_grad)
    clip_limit = 2.0 * math.sqrt(
        float(groups * hidden_units * features + router_cot.shape[0] * features)
    )
    factor = jnp.minimum(1.0, clip_limit / (jnp.sqrt(total_square) + norm_eps))
    states = adam_update(
        factor * decode(moved_gradient, rows),
        decode(early_first, rows),
        decode(early_second, rows),
        decode(early_master, rows),
    )
    router_outs = adam_update(factor * router_grad, router_first, router_second, router_master)
    sent = [encode(jnp.take(member, partner, axis=0)) for member in (states[0], states[1], states[2])]
    moved = [from_pieces(decode(exchange(payload), rows)) for payload in sent]
    moved_weight = regather(moved[0].astype(jnp.bfloat16))
    return (
        moved_weight[None],
        moved[0][None],
        moved[1][None],
        moved[2][None],
        router_outs[0],
        router_outs[1],
        router_outs[2],
    )


def solution(mesh):
    in_specs = (
        P("expert", "dp", None),
        P("expert", "dp", None),
        P("expert", "dp"),
        P("expert", "dp", None),
        P("expert", "dp", None),
        P("expert", "dp", None),
        P(("dp", "expert"), None),
        P(None, ("dp", "expert")),
        P(),
        P(),
        P(),
        P(),
    )
    out_specs = (
        P("expert", None, None),
        P("expert", "dp", None),
        P("expert", "dp", None),
        P("expert", "dp", None),
        P(),
        P(),
        P(),
    )
    return jax.shard_map(
        on_device, mesh=mesh, in_specs=in_specs, out_specs=out_specs, check_vma=False
    )
```
